768 devices in a mesh: gx: 96 (over y, z), gy: 8 (over x, core).
Axes of the slice: x: 4, y: 8, z: 12, core: 2. Of those that a mesh axis runs over, the one named last changes fastest.
Arguments:
- velocity: float32 [3, 1152, 512, 256], P(None, 'gx', 'gy'), may hold values from -6 to 6
- target: float32 [3, 393216], P(None, ('gx', 'gy')), may hold values from -6 to 6
- weights: float32 [3, 6, 393216], P(None, None, ('gx', 'gy')), may hold values from 0.02 to 0.34
- corners: int32 [3, 393216], P(None, ('gx', 'gy')), may hold values from 0 to 250, as said below
- dest: int32 [393216, 1], P(('gx', 'gy')), may hold values from 0 to 95; in each aligned block of 512 rows (0 to 511, 512 to 1023, ...) at most 12 rows name the same one
Outputs:
- velocity_next: float32 [3, 1152, 512, 256], P(None, 'gx', 'gy')
- marker_force: float32 [3, 393216], P(None, ('gx', 'gy'))
The draws below stay inside these ranges and needn't reach their ends.
Inputs may be any that keep to these rules, and one draw needn't show every extreme that they name: Each corner keeps its 6-cell box inside one device's block: corners[0] is at most 6, corners[1] at most 58, corners[2] at most 250. `dest`: among the markers of one device, at most 12 name the same streamwise index.
All inputs are finite; a program needn't handle non-finite values.
Results may differ from the reference program's by a relative error of at most 0.000071.
Values sent between devices are 32-bit elements; how exact they have to be, the bound alone decides.
A program may use at most 128 MiB of HBM per device.

```python
import math
import jax
import jax.numpy as jnp
import numpy as np
from jax import lax

CX = 12
CY = 64
CZ = 256
MARK_DEV = 512
CAP = 12
NX = 1152
NY = 512
NZ = 256
MARKERS = 393216
N_GX = 96
N_GY = 8


def draw_corners(key, part):
    upper = jnp.array([CX - 5, CY - 5, CZ - 5], jnp.int32)[:, None]
    return jax.random.randint(key, (3, MARKERS), 0, upper, dtype=jnp.int32)


def level_of(stream_key, shape, shards, smallest, largest):
    loudness, own = 1.0, jax.random.fold_in(stream_key, 6)
    for position, blocks in shards:
        heights = jnp.exp(jax.random.uniform(jax.random.fold_in(own, position), (blocks,), jnp.float32, smallest / len(shards), largest / len(shards)))
        loudness = loudness * jnp.repeat(heights, shape[position] // blocks).reshape([-1 if axis == position else 1 for axis in range(len(shape))])
    return loudness


def routed_block(key, own, number, rows, count, top, limit, lean):
    sequence = jax.random.permutation(key, count)
    packed, ordinary = shares(count, rows * top, limit, lean, True), shares(count, rows * top, limit, lean, False)
    places = jnp.arange(count)

    def named(sizes, turn):
        used = int((sizes > 0).sum())
        fixed = max(1, used // 4)
        shifted = fixed + (places - fixed + turn * (used - fixed)) % max(1, count - fixed)
        return jnp.zeros((count,), jnp.int32).at[sequence[jnp.where(places < fixed, places, shifted)]].set(jnp.asarray(sizes, jnp.int32))

    sizes = jnp.where(number % 4 == 0, named(packed, number // 4), named(ordinary, number - number // 4 - 1))
    mixed = jax.random.permutation(jax.random.fold_in(own, 3), count)
    giver, receiver = mixed[0:count // 2 * 2:2], mixed[1:count // 2 * 2:2]
    slack = jnp.minimum(sizes[giver] - 1, limit - sizes[receiver]) // 2
    slack = jnp.where((giver == sequence[0]) | (receiver == sequence[0]) | (sizes[receiver] == 0), 0, jnp.maximum(slack, 0))
    shifted = jax.random.randint(jax.random.fold_in(own, 4), (count // 2,), 0, 1 << 20) % (slack + 1)
    sizes = sizes.at[giver].add(-shifted).at[receiver].add(shifted)
    labels = jnp.searchsorted(jnp.cumsum(sizes), jnp.arange(rows * top), side="right").astype(jnp.int32)
    grid = labels.reshape(top, rows).T
    grid = grid[jax.random.permutation(jax.random.fold_in(own, 1), rows)]
    turn = jax.random.randint(jax.random.fold_in(own, 2), (rows, 1), 0, top)
    return jnp.take_along_axis(grid, (jnp.arange(top)[None, :] + turn) % top, axis=1)


def shares(amount, total, reach, slope, full):
    weights = [(1 << 20) // math.isqrt(standing ** slope) + 1 for standing in range(1, amount + 1)]
    largest = reach if full else min(reach, max(-(-total // amount), total * weights[0] // sum(weights)))
    least = 1 if total - largest >= amount - 1 else 0
    holding, spare = [largest] + [least] * (amount - 1), total - largest - least * (amount - 1)
    while spare > 0:
        movable = [i for i in range(1, amount) if holding[i] < largest] or [i for i in range(1, amount) if holding[i] < reach]
        whole, budget = sum([weights[i] for i in movable]), spare
        for i in movable:
            addition = min(reach - holding[i], max(1, budget * weights[i] // whole), spare)
            holding[i] = holding[i] + addition
            spare = spare - addition
    return np.array(holding)


def noise(rng, extent, scale, limit, shards=(), kind=jnp.bfloat16):
    gain = level_of(rng, extent, shards, -0.22, 0.18) if shards else 1.0
    values = jax.random.normal(rng, extent, jnp.float32) * scale * gain
    return jnp.minimum(jnp.maximum(values, -limit), limit).astype(kind)


def setup_inputs(seed: int = 0) -> dict:
    arg_keys = jax.random.split(jax.random.key(seed), 6)
    velocity = noise(arg_keys[0], (3, NX, NY, NZ), 1.0, 6.0, ((1, 96), (2, 8)), jnp.float32)
    target = noise(arg_keys[1], (3, MARKERS), 1.0, 6.0, ((1, 768),), jnp.float32)
    weights = jnp.clip(0.02 + 0.32 * jax.random.uniform(arg_keys[2], (3, 6, MARKERS), jnp.float32) ** level_of(arg_keys[2], (3, 6, MARKERS), ((2, 768),), -0.2, 0.2), 0.02, 0.34)
    corners = draw_corners(jax.random.fold_in(arg_keys[5], 71), 0)
    dest_keys = jax.random.split(jax.random.fold_in(arg_keys[4], 1), MARKERS // MARK_DEV)
    dest_turns = jax.random.permutation(jax.random.fold_in(arg_keys[4], 3), MARKERS // MARK_DEV)
    dest = jax.vmap(lambda own, number: routed_block(jax.random.fold_in(arg_keys[4], 2), own, number, MARK_DEV, N_GX, 1, CAP, 2))(dest_keys, dest_turns).reshape((MARKERS, 1))
    return dict(velocity=velocity, target=target, weights=weights, corners=corners, dest=dest)


diffusion = 0.4


def reference(velocity, target, weights, corners, dest):
    marker_ids = jnp.arange(MARKERS, dtype=jnp.int32)
    wall_row = (marker_ids // MARK_DEV) % N_GY
    start_x = (dest[:, 0] * CX + corners[0]).astype(jnp.int32)
    start_y = (wall_row * CY + corners[1]).astype(jnp.int32)
    start_z = corners[2].astype(jnp.int32)
    zero = jnp.zeros((), jnp.int32)

    def sample(px, py, pz, wx, wy, wz):
        box = lax.dynamic_slice(velocity, (zero, px, py, pz), (3, 6, 6, 6))
        return jnp.einsum("cabd,a,b,d->c", box, wx, wy, wz, precision=lax.Precision.HIGHEST)

    interpolated = jax.vmap(sample)(start_x, start_y, start_z, weights[0].T, weights[1].T, weights[2].T)
    marker_force = target - interpolated.T

    def add_box(index, field):
        px = start_x[index]
        py = start_y[index]
        pz = start_z[index]
        wx = weights[0, :, index]
        wy = weights[1, :, index]
        wz = weights[2, :, index]
        force = marker_force[:, index]
        box = force[:, None, None, None] * wx[None, :, None, None] * wy[None, None, :, None] * wz[None, None, None, :]
        current = lax.dynamic_slice(field, (zero, px, py, pz), (3, 6, 6, 6))
        return lax.dynamic_update_slice(field, current + box, (zero, px, py, pz))

    spread = lax.fori_loop(0, MARKERS, add_box, jnp.zeros_like(velocity))
    rhs = velocity + spread
    padded_y = jnp.pad(rhs, ((0, 0), (0, 0), (1, 1), (0, 0)))
    neighbours = padded_y[:, :, 2:] + padded_y[:, :, :-2]
    neighbours = neighbours + jnp.roll(rhs, 1, 1) + jnp.roll(rhs, -1, 1)
    neighbours = neighbours + jnp.roll(rhs, 1, 3) + jnp.roll(rhs, -1, 3)
    velocity_next = (rhs + diffusion * neighbours) / (1.0 + 6.0 * diffusion)
    return velocity_next, marker_force
```

```python
import functools
import math

import jax
import jax.numpy as jnp
from jax import lax
from jax.experimental import pallas as pl
from jax.experimental.pallas import tpu as pltpu
from jax.sharding import PartitionSpec as P

MESH = pl.DeviceIdType.MESH
F32, BF16 = jnp.float32, jnp.bfloat16
GROUPS, PER_ROW = 3, 4
CAP = GROUPS * PER_ROW
DIFFUSION = 0.4
YPAD = 40


def nn(a, b):
    return lax.dot_general(a, b, (((1,), (0,)), ((), ())), preferred_element_type=F32)


def nt(a, b):
    return lax.dot_general(a, b, (((1,), (1,)), ((), ())), preferred_element_type=F32)


def halves(value):
    high = value.astype(BF16)
    return high, (value - high.astype(F32)).astype(BF16)


def chunks(total, size):
    return [(at, min(size, total - at)) for at in range(0, total, size)]


def far(step, length):
    half = length // 2
    odd = lax.rem(step, 2)
    return lax.rem(half + length + lax.div(step, 2) * (1 - odd) - lax.div(step + 1, 2) * odd, length)


def exchange_kernel(
    n, ng, ny, nz,
    velocity, target, weights, corners, dest,
    rhs_out, xhalo, yhalo, force_out,
    v, vhi, vlo, send, recv, pay, onehot, lists, fields, zhi, zlo, wy, wx, tgt, force,
    turned, back, returned, ehi, elo, wxf, xedge, yedge, bhi, blo, rhs,
    vsem, osem, s1, r1, s2, r2, hs, hr,
):
    me, row = lax.axis_index("gx"), lax.axis_index("gy")
    my_y, my_z = lax.div(me, nz), lax.rem(me, nz)
    _, cells_x, cells_y, cells_z = v.shape
    owned = target.shape[1]
    slots = CAP * n
    inner = cells_x - 2

    def peer_of(step):
        py = lax.rem(my_y + far(lax.rem(step, ny), ny), ny)
        pz = lax.rem(my_z + far(lax.div(step, ny), nz), nz)
        return py * nz + pz

    barrier = pltpu.get_barrier_semaphore()

    def greet(step, carry):
        pl.semaphore_signal(barrier, inc=1, device_id={"gx": peer_of(step)}, device_id_type=MESH)
        return carry

    lax.fori_loop(0, n - 1, greet, 0)

    @pl.when(row > 0)
    def _():
        pl.semaphore_signal(barrier, inc=1, device_id={"gy": row - 1}, device_id_type=MESH)

    @pl.when(row < ng - 1)
    def _():
        pl.semaphore_signal(barrier, inc=1, device_id={"gy": row + 1}, device_id_type=MESH)

    load = pltpu.make_async_copy(velocity, v, vsem)
    load.start()

    wanted = dest[...]
    names = lax.broadcasted_iota(jnp.int32, (n, owned), 0) == wanted
    ones = jnp.where(names, 1.0, 0.0)
    earlier = lax.broadcasted_iota(jnp.int32, (owned, owned), 0) < lax.broadcasted_iota(
        jnp.int32, (owned, owned), 1
    )
    rank = nn(ones.astype(BF16), jnp.where(earlier, 1.0, 0.0).astype(BF16))
    rank = jnp.where(names, rank, -1.0)
    for i in range(PER_ROW):
        for g in range(GROUPS):
            at = (i * GROUPS + g) * n
            k = float(g * PER_ROW + i)
            onehot[at : at + n, :] = jnp.where(rank == k, 1.0, 0.0).astype(BF16)

    pay[...] = jnp.zeros_like(pay)
    pay[0:3, :] = target[...]
    pay[3:6, :] = corners[...].astype(F32)
    for d in range(3):
        pay[8 * (d + 1) : 8 * (d + 1) + 6, :] = weights[d]
    record = pay[...]
    first = record.astype(BF16)
    rest = record - first.astype(F32)
    second = rest.astype(BF16)
    third = (rest - second.astype(F32)).astype(BF16)
    packed = jnp.zeros((GROUPS * n, 128), F32)
    for i in range(PER_ROW):
        rows = onehot[i * GROUPS * n : (i + 1) * GROUPS * n, :]
        for piece in (first, second, third):
            parts = [piece if j == i else jnp.zeros_like(piece) for j in range(PER_ROW)]
            packed = packed + nt(rows, jnp.concatenate(parts, axis=0))
    for g in range(GROUPS):
        send[:, g, :] = packed[g * n : (g + 1) * n, :]

    expected = n - 1 + jnp.where(row > 0, 1, 0) + jnp.where(row < ng - 1, 1, 0)
    pl.semaphore_wait(barrier, expected)

    def marker_copy(peer, slot):
        return pltpu.make_async_remote_copy(
            src_ref=send.at[peer],
            dst_ref=recv.at[slot],
            send_sem=s1.at[peer],
            recv_sem=r1.at[slot],
            device_id={"gx": peer},
            device_id_type=MESH,
        )

    def ship(step, carry):
        marker_copy(peer_of(step), me).start()
        return carry

    lax.fori_loop(0, n - 1, ship, 0)
    recv[pl.ds(me, 1)] = send[pl.ds(me, 1)]

    load.wait()

    def split(step, carry):
        at = pl.ds(step * cells_y, cells_y)
        plane = v[lax.div(step, cells_x), lax.rem(step, cells_x)]
        vhi[at, :], vlo[at, :] = halves(plane)
        return carry

    lax.fori_loop(0, 3 * cells_x, split, 0)

    def land(step, carry):
        peer = peer_of(step)
        copy = marker_copy(peer, peer)
        copy.wait_recv()
        copy.wait_send()
        return carry

    lax.fori_loop(0, n - 1, land, 0)

    for g in range(GROUPS):
        block = recv[:, g, :]
        for i in range(PER_ROW):
            at = (i * GROUPS + g) * n
            lists[at : at + n, :] = block if i == 0 else pltpu.roll(block, 128 - 32 * i, 1)
    for at, size in chunks(slots, 128):
        fields[:, at : at + size] = lists[at : at + size, :].T[0:32, :]

    def window(offset, corner, length, size):
        cell = lax.broadcasted_iota(jnp.int32, (length, size), 0).astype(F32) - corner
        total = jnp.zeros((length, size), F32)
        for d in range(6):
            total = jnp.where(cell == float(d), offset(d), total)
        return total

    for at, size in chunks(slots, 128):
        lanes = slice(at, at + size)
        zhi[:, lanes], zlo[:, lanes] = halves(
            window(lambda d: fields[24 + d : 25 + d, lanes], fields[5:6, lanes], cells_z, size)
        )
        wy[:, lanes] = window(
            lambda d: fields[16 + d : 17 + d, lanes], fields[4:5, lanes], cells_y, size
        )
        along = window(lambda d: fields[8 + d : 9 + d, lanes], fields[3:4, lanes], 16, size)
        for x in range(cells_x):
            wx[x, :, lanes] = jnp.broadcast_to(along[x : x + 1, :], (8, size))
        for c in range(3):
            tgt[c, :, lanes] = jnp.broadcast_to(fields[c : c + 1, lanes], (8, size))

    def sample(c, carry):
        at = pl.ds(c * cells_x * cells_y, cells_x * cells_y)
        for start, size in chunks(slots, 256):
            lanes = slice(start, start + size)
            along = nn(vhi[at, :], zhi[:, lanes])
            along = along + nn(vhi[at, :], zlo[:, lanes])
            along = along + nn(vlo[at, :], zhi[:, lanes])
            along = along.reshape(cells_x, cells_y // 8, 8, size)
            across = jnp.sum(along * wy[:, lanes].reshape(1, cells_y // 8, 8, size), axis=1)
            across = jnp.sum(across * wx[:, :, lanes], axis=0)
            force[c, :, lanes] = tgt[c, :, lanes] - jnp.sum(across, axis=0, keepdims=True)
        return carry

    lax.fori_loop(0, 3, sample, 0)

    for at, size in chunks(slots, 128):
        three = [force[c, 0:1, at : at + size] for c in range(3)]
        three.append(jnp.zeros((125, size), F32))
        turned[at : at + size, :] = jnp.concatenate(three, axis=0).T
    gathered = turned[0:n, :]
    for b in range(1, CAP):
        gathered = gathered + pltpu.roll(turned[b * n : (b + 1) * n, :], 8 * b, 1)
    back[:, 0, :] = gathered

    def force_copy(peer, slot):
        return pltpu.make_async_remote_copy(
            src_ref=back.at[peer],
            dst_ref=returned.at[slot],
            send_sem=s2.at[peer],
            recv_sem=r2.at[slot],
            device_id={"gx": peer},
            device_id_type=MESH,
        )

    def answer(step, carry):
        force_copy(peer_of(step), me).start()
        return carry

    lax.fori_loop(0, n - 1, answer, 0)
    returned[pl.ds(me, 1)] = back[pl.ds(me, 1)]

    plane_rows = 3 * cells_y
    for c in range(3):
        for side, x in ((0, 0), (1, cells_x - 1)):
            rows = slice(side * plane_rows + c * cells_y, side * plane_rows + (c + 1) * cells_y)
            scaled = (wx[x] * force[c])[None]
            box = wy[...].reshape(cells_y // 8, 8, slots) * scaled
            ehi[rows, :], elo[rows, :] = halves(box.reshape(cells_y, slots))
        for x in range(cells_x):
            wxf[c * cells_x + x : c * cells_x + x + 1, :] = wx[x, 0:1, :] * force[c, 0:1, :]
    wxf[3 * cells_x :, :] = jnp.zeros((48 - 3 * cells_x, slots), F32)
    for side, y in ((0, 0), (1, cells_y - 1)):
        rows = slice(2 * plane_rows + 48 * side, 2 * plane_rows + 48 * (side + 1))
        ehi[rows, :], elo[rows, :] = halves(wxf[...] * wy[y : y + 1, :])
    faces = nt(ehi[...], zhi[...]) + nt(ehi[...], zlo[...]) + nt(elo[...], zhi[...])
    for side, x, y in ((0, 0, 0), (1, cells_x - 1, cells_y - 1)):
        for c in range(3):
            rows = slice(side * plane_rows + c * cells_y, side * plane_rows + (c + 1) * cells_y)
            xedge[side, c] = faces[rows] + v[c, x]
            at = 2 * plane_rows + 48 * side + c * cells_x
            yedge[side, c * cells_x : (c + 1) * cells_x, :] = faces[at : at + cells_x] + v[c, :, y, :]
        yedge[side, 3 * cells_x :, :] = jnp.zeros((YPAD - 3 * cells_x, cells_z), F32)

    def face_copy(source, halo, side, semaphore, to):
        return pltpu.make_async_remote_copy(
            src_ref=source.at[side],
            dst_ref=halo.at[1 - side],
            send_sem=hs.at[semaphore],
            recv_sem=hr.at[semaphore],
            device_id=to,
            device_id_type=MESH,
        )

    down = face_copy(xedge, xhalo, 0, 0, {"gx": lax.rem(me + n - 1, n)})
    up = face_copy(xedge, xhalo, 1, 1, {"gx": lax.rem(me + 1, n)})
    below = face_copy(yedge, yhalo, 0, 2, {"gy": jnp.maximum(row - 1, 0)})
    above = face_copy(yedge, yhalo, 1, 3, {"gy": jnp.minimum(row + 1, ng - 1)})
    down.start()
    up.start()

    @pl.when(row > 0)
    def _():
        below.start()

    @pl.when(row < ng - 1)
    def _():
        above.start()

    def edge_out(c, side, x):
        return pltpu.make_async_copy(xedge.at[side, c], rhs_out.at[c, x], osem.at[2 * c + side])

    for c in range(3):
        edge_out(c, 0, 0).start()
        edge_out(c, 1, cells_x - 1).start()

    def inner_out(c):
        return pltpu.make_async_copy(
            rhs.at[c], rhs_out.at[c, pl.ds(1, inner)], osem.at[6 + c]
        )

    def spread(c, carry):
        def outer(x, carry):
            scaled = (wx[x + 1] * force[c])[None]
            box = (wy[...].reshape(cells_y // 8, 8, slots) * scaled).reshape(cells_y, slots)
            at = pl.ds(x * cells_y, cells_y)
            bhi[at, :], blo[at, :] = halves(box)
            return carry

        lax.fori_loop(0, inner, outer, 0)
        total = nt(bhi[...], zhi[...]) + nt(bhi[...], zlo[...]) + nt(blo[...], zhi[...])
        rhs[c] = v[c, 1 : cells_x - 1] + total.reshape(inner, cells_y, cells_z)
        inner_out(c).start()
        return carry

    lax.fori_loop(0, 3, spread, 0)

    def settle(step, carry):
        peer = peer_of(step)
        copy = force_copy(peer, peer)
        copy.wait_recv()
        copy.wait_send()
        return carry

    lax.fori_loop(0, n - 1, settle, 0)

    found = jnp.zeros((24, owned), F32)
    answers = returned[:, 0, :].T
    for i in range(PER_ROW):
        for g in range(GROUPS):
            b = i * GROUPS + g
            part = answers[8 * b : 8 * b + 8, :]
            first = part.astype(BF16).astype(F32)
            rest = part - first
            second = rest.astype(BF16).astype(F32)
            stack = jnp.concatenate([first, second, rest - second], axis=0).astype(BF16)
            found = found + nn(stack, onehot[b * n : (b + 1) * n, :])
    force_out[...] = found[0:8] + found[8:16] + found[16:24]

    for c in range(3):
        edge_out(c, 0, 0).wait()
        edge_out(c, 1, cells_x - 1).wait()
        inner_out(c).wait()
    down.wait()
    up.wait()

    @pl.when(row > 0)
    def _():
        below.wait_send()
        above.wait_recv()

    @pl.when(row < ng - 1)
    def _():
        above.wait_send()
        below.wait_recv()


def sweep_kernel(ng, rhs, xhalo, yhalo, out):
    row = lax.axis_index("gy")
    c = pl.program_id(0)
    _, cells_x, cells_y, cells_z = rhs.shape
    last = lax.broadcasted_iota(jnp.int32, (cells_y, cells_z), 0)
    for x in range(cells_x):
        here = rhs[0, x]
        total = xhalo[0, 0] if x == 0 else rhs[0, x - 1]
        total = total + (xhalo[1, 0] if x == cells_x - 1 else rhs[0, x + 1])
        total = total + pltpu.roll(here, 1, 1) + pltpu.roll(here, cells_z - 1, 1)
        at = c * cells_x + x
        lower = jnp.where(row == 0, 0.0, yhalo[0, pl.ds(at, 1), :])
        upper = jnp.where(row == ng - 1, 0.0, yhalo[1, pl.ds(at, 1), :])
        total = total + jnp.where(last == 0, lower, pltpu.roll(here, 1, 0))
        total = total + jnp.where(last == cells_y - 1, upper, pltpu.roll(here, cells_y - 1, 0))
        out[0, x] = (here + DIFFUSION * total) * (1.0 / (1.0 + 6.0 * DIFFUSION))


def per_device(velocity, target, weights, corners, dest):
    n, ng = lax.axis_size("gx"), lax.axis_size("gy")
    ny = next(d for d in range(math.isqrt(n), 0, -1) if n % d == 0)
    nz = n // ny
    _, cells_x, cells_y, cells_z = velocity.shape
    owned = target.shape[1]
    slots = CAP * n
    inner = cells_x - 2
    whole = pl.BlockSpec(memory_space=pltpu.VMEM)
    anywhere = pl.BlockSpec(memory_space=pl.ANY)
    vmem, dma = pltpu.VMEM, pltpu.SemaphoreType.DMA
    field = jax.ShapeDtypeStruct(velocity.shape, F32)
    xhalos = jax.ShapeDtypeStruct((2, 3, cells_y, cells_z), F32)
    yhalos = jax.ShapeDtypeStruct((2, YPAD, cells_z), F32)
    flat = 3 * cells_x * cells_y
    edges = 6 * cells_y + 96
    rhs, xhalo, yhalo, force = pl.pallas_call(
        functools.partial(exchange_kernel, n, ng, ny, nz),
        out_shape=(field, xhalos, yhalos, jax.ShapeDtypeStruct((8, owned), F32)),
        in_specs=[anywhere, whole, whole, whole, whole],
        out_specs=(anywhere, anywhere, anywhere, whole),
        scratch_shapes=[
            vmem(velocity.shape, F32),
            vmem((flat, cells_z), BF16),
            vmem((flat, cells_z), BF16),
            vmem((n, GROUPS, 128), F32),
            vmem((n, GROUPS, 128), F32),
            vmem((32, owned), F32),
            vmem((slots, owned), BF16),
            vmem((slots, 128), F32),
            vmem((32, slots), F32),
            vmem((cells_z, slots), BF16),
            vmem((cells_z, slots), BF16),
            vmem((cells_y, slots), F32),
            vmem((cells_x, 8, slots), F32),
            vmem((3, 8, slots), F32),
            vmem((3, 8, slots), F32),
            vmem((slots, 128), F32),
            vmem((n, 1, 128), F32),
            vmem((n, 1, 128), F32),
            vmem((edges, slots), BF16),
            vmem((edges, slots), BF16),
            vmem((48, slots), F32),
            vmem((2, 3, cells_y, cells_z), F32),
            vmem((2, YPAD, cells_z), F32),
            vmem((inner * cells_y, slots), BF16),
            vmem((inner * cells_y, slots), BF16),
            vmem((3, inner, cells_y, cells_z), F32),
            dma,
            dma((9,)),
            dma((n,)),
            dma((n,)),
            dma((n,)),
            dma((n,)),
            dma((4,)),
            dma((4,)),
        ],
        compiler_params=pltpu.CompilerParams(
            collective_id=0, has_side_effects=True, vmem_limit_bytes=50 * 1024 * 1024
        ),
        name="exchange",
    )(velocity, target, weights, corners, dest.reshape(1, owned))
    moved = pl.pallas_call(
        functools.partial(sweep_kernel, ng),
        grid=(3,),
        out_shape=field,
        in_specs=[
            pl.BlockSpec((1, cells_x, cells_y, cells_z), lambda c: (c, 0, 0, 0)),
            pl.BlockSpec((2, 1, cells_y, cells_z), lambda c: (0, c, 0, 0)),
            pl.BlockSpec((2, YPAD, cells_z), lambda c: (0, 0, 0)),
        ],
        out_specs=pl.BlockSpec((1, cells_x, cells_y, cells_z), lambda c: (c, 0, 0, 0)),
        compiler_params=pltpu.CompilerParams(vmem_limit_bytes=16 * 1024 * 1024),
        name="sweep",
    )(rhs, xhalo, yhalo)
    return moved, force[0:3]


def solution(mesh):
    in_specs = (
        P(None, "gx", "gy", None),
        P(None, ("gx", "gy")),
        P(None, None, ("gx", "gy")),
        P(None, ("gx", "gy")),
        P(("gx", "gy"), None),
    )
    out_specs = (P(None, "gx", "gy", None), P(None, ("gx", "gy")))
    return jax.shard_map(
        per_device, mesh=mesh, in_specs=in_specs, out_specs=out_specs, check_vma=False
    )
```

```python
import functools

import jax
import jax.numpy as jnp
from jax import lax
from jax.experimental import pallas as pl
from jax.experimental.pallas import tpu as pltpu
from jax.sharding import PartitionSpec as P

MESH = pl.DeviceIdType.MESH
F32, BF16 = jnp.float32, jnp.bfloat16
GROUPS, PER_ROW = 3, 4
CAP = GROUPS * PER_ROW
DIFFUSION = 0.4
YPAD = 16


def nn(a, b):
    return lax.dot_general(a, b, (((1,), (0,)), ((), ())), preferred_element_type=F32)


def nt(a, b):
    return lax.dot_general(a, b, (((1,), (1,)), ((), ())), preferred_element_type=F32)


def halves(value):
    high = value.astype(BF16)
    return high, (value - high.astype(F32)).astype(BF16)


def chunks(total, size):
    return [(at, min(size, total - at)) for at in range(0, total, size)]


def exchange_kernel(
    n, ng,
    velocity, target_in, weights_in, corners_in, dest_in,
    rhs_out, xhalo, yhalo, force_out,
    v, rhs, own, target, weights, corners, dest, vhi, vlo, send, recv, pay, onehot, lists, fields, zhi, zlo, wy,
    wx, tgt, force, turned, back, returned, ehi, elo, wxf, yedge, bhi0, blo0, bhi1, blo1,
    vsem, isem, osem, s1, r1, s2, r2, hs, hr,
):
    me, row = lax.axis_index("gx"), lax.axis_index("gy")
    _, cells_x, cells_y, cells_z = v.shape
    owned = target.shape[1]
    slots = CAP * n
    inner = cells_x - 2
    half = n // 2

    def ahead(offset):
        peer = me + offset
        return jnp.where(peer >= n, peer - n, peer)

    def all_peers(act):
        act(half)

        def two(step, carry):
            act(half - step)
            act(half + step)
            return carry

        lax.fori_loop(1, half, two, 0)

    barrier = pltpu.get_barrier_semaphore()

    def greet(offset):
        pl.semaphore_signal(barrier, inc=1, device_id={"gx": ahead(offset)}, device_id_type=MESH)

    inputs = [
        pltpu.make_async_copy(source, held, isem.at[i])
        for i, (source, held) in enumerate(
            ((dest_in, dest), (target_in, target), (corners_in, corners), (weights_in, weights))
        )
    ]
    for copy in inputs:
        copy.start()
    load = pltpu.make_async_copy(velocity, v, vsem)
    load.start()
    all_peers(greet)

    @pl.when(row > 0)
    def _():
        pl.semaphore_signal(barrier, inc=1, device_id={"gy": row - 1}, device_id_type=MESH)

    @pl.when(row < ng - 1)
    def _():
        pl.semaphore_signal(barrier, inc=1, device_id={"gy": row + 1}, device_id_type=MESH)

    inputs[0].wait()

    wanted = dest[...]
    names = lax.broadcasted_iota(jnp.int32, (n, owned), 0) == wanted
    ones = jnp.where(names, 1.0, 0.0)
    earlier = lax.broadcasted_iota(jnp.int32, (owned, owned), 0) < lax.broadcasted_iota(
        jnp.int32, (owned, owned), 1
    )
    rank = nn(ones.astype(BF16), jnp.where(earlier, 1.0, 0.0).astype(BF16))
    rank = jnp.where(names, rank, -1.0)
    for i in range(PER_ROW):
        for g in range(GROUPS):
            at = (i * GROUPS + g) * n
            k = float(g * PER_ROW + i)
            onehot[at : at + n, :] = jnp.where(rank == k, 1.0, 0.0).astype(BF16)

    for copy in inputs[1:]:
        copy.wait()

    pay[...] = jnp.zeros_like(pay)
    pay[0:3, :] = target[...]
    pay[3:6, :] = corners[...].astype(F32)
    for d in range(3):
        pay[8 * (d + 1) : 8 * (d + 1) + 6, :] = weights[d]
    record = pay[...]
    first = record.astype(BF16)
    rest = record - first.astype(F32)
    second = rest.astype(BF16)
    third = (rest - second.astype(F32)).astype(BF16)
    packed = jnp.zeros((GROUPS * n, 128), F32)
    for i in range(PER_ROW):
        rows = onehot[i * GROUPS * n : (i + 1) * GROUPS * n, :]
        for piece in (first, second, third):
            parts = [piece if j == i else jnp.zeros_like(piece) for j in range(PER_ROW)]
            packed = packed + nt(rows, jnp.concatenate(parts, axis=0))
    for g in range(GROUPS):
        send[:, g, :] = packed[g * n : (g + 1) * n, :]

    expected = n - 1 + jnp.where(row > 0, 1, 0) + jnp.where(row < ng - 1, 1, 0)
    pl.semaphore_wait(barrier, expected)

    def ship(offset):
        peer = ahead(offset)
        pltpu.make_async_remote_copy(
            src_ref=send.at[peer],
            dst_ref=recv.at[n - offset],
            send_sem=s1,
            recv_sem=r1,
            device_id={"gx": peer},
            device_id_type=MESH,
        ).start()

    all_peers(ship)
    recv[0:1] = send[pl.ds(me, 1)]

    load.wait()

    def split(step, carry):
        at = pl.ds(step * cells_y, cells_y)
        plane = v[lax.div(step, cells_x), lax.rem(step, cells_x)]
        vhi[at, :], vlo[at, :] = halves(plane)
        return carry

    lax.fori_loop(0, 3 * cells_x, split, 0)

    def all_of(source, landed, sent, arrived):
        return pltpu.make_async_remote_copy(
            src_ref=source.at[pl.ds(0, n - 1)],
            dst_ref=landed.at[pl.ds(1, n - 1)],
            send_sem=sent,
            recv_sem=arrived,
            device_id={"gx": ahead(1)},
            device_id_type=MESH,
        )

    all_of(send, recv, s1, r1).wait_recv()

    for g in range(GROUPS):
        block = recv[:, g, :]
        for i in range(PER_ROW):
            at = (i * GROUPS + g) * n
            lists[at : at + n, :] = block if i == 0 else pltpu.roll(block, 128 - 32 * i, 1)
    for at, size in chunks(slots, 128):
        fields[:, at : at + size] = lists[at : at + size, :].T[0:32, :]

    def window(offset, corner, length, size):
        cell = lax.broadcasted_iota(jnp.int32, (length, size), 0).astype(F32) - corner
        total = jnp.zeros((length, size), F32)
        for d in range(6):
            total = jnp.where(cell == float(d), offset(d), total)
        return total

    for at, size in chunks(slots, 128):
        lanes = slice(at, at + size)
        zhi[:, lanes], zlo[:, lanes] = halves(
            window(lambda d: fields[24 + d : 25 + d, lanes], fields[5:6, lanes], cells_z, size)
        )
        wy[:, lanes] = window(
            lambda d: fields[16 + d : 17 + d, lanes], fields[4:5, lanes], cells_y, size
        )
        along = window(lambda d: fields[8 + d : 9 + d, lanes], fields[3:4, lanes], 16, size)
        for x in range(cells_x):
            wx[x, :, lanes] = jnp.broadcast_to(along[x : x + 1, :], (8, size))
        for c in range(3):
            tgt[c, :, lanes] = jnp.broadcast_to(fields[c : c + 1, lanes], (8, size))

    def sample(c, carry):
        at = pl.ds(c * cells_x * cells_y, cells_x * cells_y)
        for start, size in chunks(slots, 256):
            lanes = slice(start, start + size)
            along = nn(vhi[at, :], zhi[:, lanes])
            along = along + nn(vhi[at, :], zlo[:, lanes])
            along = along + nn(vlo[at, :], zhi[:, lanes])
            along = along.reshape(cells_x, cells_y // 8, 8, size)
            across = jnp.sum(along * wy[:, lanes].reshape(1, cells_y // 8, 8, size), axis=1)
            across = jnp.sum(across * wx[:, :, lanes], axis=0)
            force[c, :, lanes] = tgt[c, :, lanes] - jnp.sum(across, axis=0, keepdims=True)
        return carry

    lax.fori_loop(0, 3, sample, 0)

    for at, size in chunks(slots, 128):
        three = [force[c, 0:1, at : at + size] for c in range(3)]
        three.append(jnp.zeros((125, size), F32))
        turned[at : at + size, :] = jnp.concatenate(three, axis=0).T
    gathered = turned[0:n, :]
    for b in range(1, CAP):
        gathered = gathered + pltpu.roll(turned[b * n : (b + 1) * n, :], 8 * b, 1)
    back[:, 0, :] = gathered

    def answer(offset):
        pltpu.make_async_remote_copy(
            src_ref=back.at[offset],
            dst_ref=returned.at[me],
            send_sem=s2,
            recv_sem=r2,
            device_id={"gx": ahead(offset)},
            device_id_type=MESH,
        ).start()

    all_peers(answer)
    returned[pl.ds(me, 1)] = back[0:1]

    def face_copy(source, halo, semaphore, to):
        return pltpu.make_async_remote_copy(
            src_ref=source,
            dst_ref=halo,
            send_sem=hs.at[semaphore],
            recv_sem=hr.at[semaphore],
            device_id=to,
            device_id_type=MESH,
        )

    sides = ((0, 0, 0), (1, cells_x - 1, cells_y - 1))
    near_copies, below_copies, above_copies = [], [], []
    for c in range(3):
        for side, x, y in sides:
            rows = slice(side * cells_y, (side + 1) * cells_y)
            box = wy[...].reshape(cells_y // 8, 8, slots) * (wx[x] * force[c])[None]
            ehi[c, rows, :], elo[c, rows, :] = halves(box.reshape(cells_y, slots))
        for x in range(cells_x):
            wxf[c, x : x + 1, :] = wx[x, 0:1, :] * force[c, 0:1, :]
        wxf[c, cells_x:, :] = jnp.zeros((YPAD - cells_x, slots), F32)
        for side, x, y in sides:
            rows = slice(2 * cells_y + YPAD * side, 2 * cells_y + YPAD * (side + 1))
            ehi[c, rows, :], elo[c, rows, :] = halves(wxf[c] * wy[y : y + 1, :])
        faces = nt(ehi[c], zhi[...]) + nt(ehi[c], zlo[...]) + nt(elo[c], zhi[...])
        for side, x, y in sides:
            rhs[c, x] = faces[side * cells_y : (side + 1) * cells_y] + v[c, x]
            at = 2 * cells_y + YPAD * side
            yedge[side, c, 0:cells_x, :] = faces[at : at + cells_x] + v[c, :, y, :]
            yedge[side, c, cells_x:, :] = jnp.zeros((YPAD - cells_x, cells_z), F32)
        down = face_copy(rhs.at[c, 0], xhalo.at[1, c], 4 * c, {"gx": ahead(n - 1)})
        up = face_copy(rhs.at[c, cells_x - 1], xhalo.at[0, c], 4 * c + 1, {"gx": ahead(1)})
        below = face_copy(
            yedge.at[0, c], yhalo.at[1, c], 4 * c + 2, {"gy": jnp.maximum(row - 1, 0)}
        )
        above = face_copy(
            yedge.at[1, c], yhalo.at[0, c], 4 * c + 3, {"gy": jnp.minimum(row + 1, ng - 1)}
        )
        down.start()
        up.start()
        near_copies += [down, up]
        below_copies.append(below)
        above_copies.append(above)

        @pl.when(row > 0)
        def _():
            below.start()

        @pl.when(row < ng - 1)
        def _():
            above.start()

    outward = [
        pltpu.make_async_copy(rhs.at[:, x], rhs_out.at[:, x], osem.at[i])
        for i, x in enumerate((0, cells_x - 1))
    ]
    for copy in outward:
        copy.start()

    def build(c, high, low):
        for x in range(inner):
            scaled = (wx[x + 1] * force[c])[None]
            box = (wy[...].reshape(cells_y // 8, 8, slots) * scaled).reshape(cells_y, slots)
            at = slice(x * cells_y, (x + 1) * cells_y)
            high[at, :], low[at, :] = halves(box)

    buffers = ((bhi0, blo0), (bhi1, blo1))
    build(0, *buffers[0])
    for c in range(3):
        high, low = buffers[c % 2]
        total = nt(high[...], zhi[...]) + nt(high[...], zlo[...]) + nt(low[...], zhi[...])
        rhs[c, 1 : cells_x - 1] = v[c, 1 : cells_x - 1] + total.reshape(inner, cells_y, cells_z)
        middle = pl.ds(1, inner)
        copy = pltpu.make_async_copy(rhs.at[c, middle], rhs_out.at[c, middle], osem.at[2 + c])
        copy.start()
        outward.append(copy)
        if c < 2:
            build(c + 1, *buffers[(c + 1) % 2])

    all_of(back, returned, s2, r2).wait_recv()

    found = jnp.zeros((24, owned), F32)
    answers = returned[:, 0, :].T
    for i in range(PER_ROW):
        for g in range(GROUPS):
            b = i * GROUPS + g
            part = answers[8 * b : 8 * b + 8, :]
            first = part.astype(BF16).astype(F32)
            rest = part - first
            second = rest.astype(BF16).astype(F32)
            stack = jnp.concatenate([first, second, rest - second], axis=0).astype(BF16)
            found = found + nn(stack, onehot[b * n : (b + 1) * n, :])
    own[...] = found[0:8] + found[8:16] + found[16:24]
    copy = pltpu.make_async_copy(own, force_out, osem.at[5])
    copy.start()
    outward.append(copy)

    for copy in outward:
        copy.wait()
    all_of(send, recv, s1, r1).wait_send()
    all_of(back, returned, s2, r2).wait_send()
    for copy in near_copies:
        copy.wait()

    @pl.when(row > 0)
    def _():
        for below, above in zip(below_copies, above_copies):
            below.wait_send()
            above.wait_recv()

    @pl.when(row < ng - 1)
    def _():
        for below, above in zip(below_copies, above_copies):
            above.wait_send()
            below.wait_recv()


def sweep_kernel(
    ng, rhs_in, xhalo_in, yhalo_in, force_in, out, force_out, rhs, xhalo, yhalo, force, made, lsem, sem
):
    row = lax.axis_index("gy")
    _, cells_x, cells_y, cells_z = rhs.shape
    part = cells_x // 2

    def halves_of(source, held, semaphores):
        return [
            pltpu.make_async_copy(
                source.at[c, pl.ds(h * part, part)], held.at[c, pl.ds(h * part, part)], semaphores.at[2 * c + h]
            )
            for c in range(3)
            for h in range(2)
        ]

    loads = halves_of(rhs_in, rhs, lsem)
    copies = halves_of(made, out, sem)
    rows_in = pltpu.make_async_copy(yhalo_in, yhalo, lsem.at[6])
    planes_in = pltpu.make_async_copy(xhalo_in, xhalo, lsem.at[7])
    last_in = pltpu.make_async_copy(force_in, force, lsem.at[8])
    for copy in (loads[0], rows_in, planes_in, *loads[1:], last_in):
        copy.start()
    line = lax.broadcasted_iota(jnp.int32, (cells_y, cells_z), 0)
    for c in range(3):
        loads[2 * c].wait()
        if c == 0:
            rows_in.wait()
        for turn, x in enumerate([*range(1, part - 1), 0, *range(part - 1, cells_x)]):
            if x == 0 and c == 0:
                planes_in.wait()
            if x == part - 1:
                loads[2 * c + 1].wait()
            here = rhs[c, x]
            total = xhalo[0, c] if x == 0 else rhs[c, x - 1]
            total = total + (xhalo[1, c] if x == cells_x - 1 else rhs[c, x + 1])
            total = total + pltpu.roll(here, 1, 1) + pltpu.roll(here, cells_z - 1, 1)
            lower = jnp.where(row == 0, 0.0, yhalo[0, c, x : x + 1, :])
            upper = jnp.where(row == ng - 1, 0.0, yhalo[1, c, x : x + 1, :])
            total = total + jnp.where(line == 0, lower, pltpu.roll(here, 1, 0))
            total = total + jnp.where(line == cells_y - 1, upper, pltpu.roll(here, cells_y - 1, 0))
            made[c, x] = (here + DIFFUSION * total) * (1.0 / (1.0 + 6.0 * DIFFUSION))
            if turn % part == part - 1:
                copies[2 * c + turn // part].start()
    last_in.wait()
    force_out[...] = force[0:3, :]
    for copy in copies:
        copy.wait()


def per_device(velocity, target, weights, corners, dest):
    n, ng = lax.axis_size("gx"), lax.axis_size("gy")
    _, cells_x, cells_y, cells_z = velocity.shape
    owned = target.shape[1]
    slots = CAP * n
    inner = cells_x - 2
    whole = pl.BlockSpec(memory_space=pltpu.VMEM)
    outside = pl.BlockSpec(memory_space=pltpu.HBM)
    vmem, dma = pltpu.VMEM, pltpu.SemaphoreType.DMA
    field = jax.ShapeDtypeStruct(velocity.shape, F32)
    flat = 3 * cells_x * cells_y
    edges = 2 * (cells_y + YPAD)
    rhs, xhalo, yhalo, force = pl.pallas_call(
        functools.partial(exchange_kernel, n, ng),
        out_shape=(
            field,
            jax.ShapeDtypeStruct((2, 3, cells_y, cells_z), F32),
            jax.ShapeDtypeStruct((2, 3, YPAD, cells_z), F32),
            jax.ShapeDtypeStruct((8, owned), F32),
        ),
        in_specs=[outside] * 5,
        out_specs=(outside,) * 4,
        scratch_shapes=[
            vmem(velocity.shape, F32),
            vmem(velocity.shape, F32),
            vmem((8, owned), F32),
            vmem(target.shape, F32),
            vmem(weights.shape, F32),
            vmem(corners.shape, jnp.int32),
            vmem((1, owned), jnp.int32),
            vmem((flat, cells_z), BF16),
            vmem((flat, cells_z), BF16),
            vmem((n, GROUPS, 128), F32),
            vmem((n, GROUPS, 128), F32),
            vmem((32, owned), F32),
            vmem((slots, owned), BF16),
            vmem((slots, 128), F32),
            vmem((32, slots), F32),
            vmem((cells_z, slots), BF16),
            vmem((cells_z, slots), BF16),
            vmem((cells_y, slots), F32),
            vmem((cells_x, 8, slots), F32),
            vmem((3, 8, slots), F32),
            vmem((3, 8, slots), F32),
            vmem((slots, 128), F32),
            vmem((n, 1, 128), F32),
            vmem((n, 1, 128), F32),
            vmem((3, edges, slots), BF16),
            vmem((3, edges, slots), BF16),
            vmem((3, YPAD, slots), F32),
            vmem((2, 3, YPAD, cells_z), F32),
            vmem((inner * cells_y, slots), BF16),
            vmem((inner * cells_y, slots), BF16),
            vmem((inner * cells_y, slots), BF16),
            vmem((inner * cells_y, slots), BF16),
            dma,
            dma((4,)),
            dma((6,)),
            dma,
            dma,
            dma,
            dma,
            dma((12,)),
            dma((12,)),
        ],
        compiler_params=pltpu.CompilerParams(
            collective_id=0, has_side_effects=True, vmem_limit_bytes=58000000
        ),
        name="exchange",
    )(velocity, target, weights, corners, dest.reshape(1, owned))
    return pl.pallas_call(
        functools.partial(sweep_kernel, ng),
        out_shape=(field, jax.ShapeDtypeStruct((3, owned), F32)),
        in_specs=[outside] * 4,
        out_specs=(outside, whole),
        scratch_shapes=[
            vmem(velocity.shape, F32),
            vmem((2, 3, cells_y, cells_z), F32),
            vmem((2, 3, YPAD, cells_z), F32),
            vmem((8, owned), F32),
            vmem(velocity.shape, F32),
            dma((9,)),
            dma((6,)),
        ],
        compiler_params=pltpu.CompilerParams(vmem_limit_bytes=58000000),
        name="sweep",
    )(rhs, xhalo, yhalo, force)


def solution(mesh):
    in_specs = (
        P(None, "gx", "gy", None),
        P(None, ("gx", "gy")),
        P(None, None, ("gx", "gy")),
        P(None, ("gx", "gy")),
        P(("gx", "gy"), None),
    )
    out_specs = (P(None, "gx", "gy", None), P(None, ("gx", "gy")))
    return jax.shard_map(
        per_device, mesh=mesh, in_specs=in_specs, out_specs=out_specs, check_vma=False
    )
```

```python
import functools
import math

import jax
import jax.numpy as jnp
from jax import lax
from jax.experimental import pallas as pl
from jax.experimental.pallas import tpu as pltpu
from jax.sharding import PartitionSpec as P

MESH = pl.DeviceIdType.MESH
F32, BF16 = jnp.float32, jnp.bfloat16
GROUPS, PER_ROW = 3, 4
CAP = GROUPS * PER_ROW
DIFFUSION = 0.4
YPAD = 16


def nn(a, b):
    return lax.dot_general(a, b, (((1,), (0,)), ((), ())), preferred_element_type=F32)


def nt(a, b):
    return lax.dot_general(a, b, (((1,), (1,)), ((), ())), preferred_element_type=F32)


def halves(value):
    high = value.astype(BF16)
    return high, (value - high.astype(F32)).astype(BF16)


def chunks(total, size):
    return [(at, min(size, total - at)) for at in range(0, total, size)]


class Order:
    def __init__(self, n):
        self.ny = next(d for d in range(math.isqrt(n), 0, -1) if n % d == 0)
        self.nz = n // self.ny
        if (self.ny, self.nz) == (8, 12):
            self.reach = (5, 5, 4, 2, 1, 2, 4, 5)
        else:
            self.reach = (0,) * self.ny
        self.near, self.far, at = [], [], 0
        for reach in self.reach:
            self.near.append(at)
            at += 2 * reach + 1
        self.split = at
        for reach in self.reach:
            self.far.append(at)
            at += self.nz - 2 * reach - 1
        self.groups = ((0, self.split), (self.split, n - self.split))
        self.own = self.near[0] + self.reach[0]

    def visit(self, me, act):
        y, z = lax.div(me, self.nz), lax.rem(me, self.nz)
        ny, nz = self.ny, self.nz
        turns = sorted(range(ny), key=lambda dy: -min(dy, ny - dy))
        for group in (1, 0):
            for dy in turns:
                reach, back = self.reach[dy], (ny - dy) % ny
                py = jnp.where(y + dy >= ny, y + dy - ny, y + dy)
                if group:
                    steps = nz - 2 * reach - 1
                    spans = [(reach + 1, steps, self.far[dy], self.far[back] + steps - 1)]
                else:
                    mid, seen = self.near[dy] + reach, self.near[back] + reach
                    skip = 1 if dy == 0 else 0
                    spans = [(skip, reach + 1 - skip, mid + skip, seen - skip)]
                    if reach:
                        spans.append((nz - reach, reach, mid - reach, seen + reach))
                for first, steps, mine, theirs in spans:

                    def one(k, carry):
                        pz = z + first + k
                        pz = jnp.where(pz >= nz, pz - nz, pz)
                        act(group, py * nz + pz, mine + k, theirs - k)
                        return carry

                    lax.fori_loop(0, steps, one, 0)


def exchange_kernel(
    n, ng,
    velocity, target_in, weights_in, corners_in, dest_in,
    rhs_out, xhalo, yhalo, force_out,
    v, rhs, own, target, weights, corners, dest, vhi, vlo, send, recv, pay, onehot, lists, fields, zhi, zlo, wy,
    wx, tgt, force, turned, back, returned, ehi, elo, wxf, yedge, bhi0, blo0, bhi1, blo1,
    vsem, isem, osem, s1, r1, s2, r2, hs, hr,
):
    me, row = lax.axis_index("gx"), lax.axis_index("gy")
    _, cells_x, cells_y, cells_z = v.shape
    owned = target.shape[1]
    slots = CAP * n
    inner = cells_x - 2
    order = Order(n)

    def ahead(offset):
        peer = me + offset
        return jnp.where(peer >= n, peer - n, peer)

    barrier = pltpu.get_barrier_semaphore()

    def greet(group, peer, mine, theirs):
        pl.semaphore_signal(barrier, inc=1, device_id={"gx": peer}, device_id_type=MESH)

    inputs = [
        pltpu.make_async_copy(source, held, isem.at[i])
        for i, (source, held) in enumerate(
            ((dest_in, dest), (target_in, target), (corners_in, corners), (weights_in, weights))
        )
    ]
    for copy in inputs:
        copy.start()
    load = pltpu.make_async_copy(velocity, v, vsem)
    load.start()
    order.visit(me, greet)

    @pl.when(row > 0)
    def _():
        pl.semaphore_signal(barrier, inc=1, device_id={"gy": row - 1}, device_id_type=MESH)

    @pl.when(row < ng - 1)
    def _():
        pl.semaphore_signal(barrier, inc=1, device_id={"gy": row + 1}, device_id_type=MESH)

    inputs[0].wait()

    wanted = dest[...]
    names = lax.broadcasted_iota(jnp.int32, (n, owned), 0) == wanted
    ones = jnp.where(names, 1.0, 0.0)
    earlier = lax.broadcasted_iota(jnp.int32, (owned, owned), 0) < lax.broadcasted_iota(
        jnp.int32, (owned, owned), 1
    )
    rank = nn(ones.astype(BF16), jnp.where(earlier, 1.0, 0.0).astype(BF16))
    rank = jnp.where(names, rank, -1.0)
    for i in range(PER_ROW):
        for g in range(GROUPS):
            at = (i * GROUPS + g) * n
            k = float(g * PER_ROW + i)
            onehot[at : at + n, :] = jnp.where(rank == k, 1.0, 0.0).astype(BF16)

    for copy in inputs[1:]:
        copy.wait()

    pay[...] = jnp.zeros_like(pay)
    pay[0:3, :] = target[...]
    pay[3:6, :] = corners[...].astype(F32)
    for d in range(3):
        pay[8 * (d + 1) : 8 * (d + 1) + 6, :] = weights[d]
    record = pay[...]
    first = record.astype(BF16)
    rest = record - first.astype(F32)
    second = rest.astype(BF16)
    third = (rest - second.astype(F32)).astype(BF16)
    packed = jnp.zeros((GROUPS * n, 128), F32)
    for i in range(PER_ROW):
        rows = onehot[i * GROUPS * n : (i + 1) * GROUPS * n, :]
        for piece in (first, second, third):
            parts = [piece if j == i else jnp.zeros_like(piece) for j in range(PER_ROW)]
            packed = packed + nt(rows, jnp.concatenate(parts, axis=0))
    for g in range(GROUPS):
        send[:, g, :] = packed[g * n : (g + 1) * n, :]

    expected = n - 1 + jnp.where(row > 0, 1, 0) + jnp.where(row < ng - 1, 1, 0)
    pl.semaphore_wait(barrier, expected)

    def ship(group, peer, mine, theirs):
        pltpu.make_async_remote_copy(
            src_ref=send.at[peer],
            dst_ref=recv.at[theirs],
            send_sem=s1,
            recv_sem=r1.at[group],
            device_id={"gx": peer},
            device_id_type=MESH,
        ).start()

    order.visit(me, ship)
    recv[order.own : order.own + 1] = send[pl.ds(me, 1)]

    load.wait()

    def split(step, carry):
        at = pl.ds(step * cells_y, cells_y)
        plane = v[lax.div(step, cells_x), lax.rem(step, cells_x)]
        vhi[at, :], vlo[at, :] = halves(plane)
        return carry

    lax.fori_loop(0, 3 * cells_x, split, 0)

    def all_of(source, landed, count, sent, arrived):
        return pltpu.make_async_remote_copy(
            src_ref=source.at[pl.ds(0, count)],
            dst_ref=landed.at[pl.ds(0, count)],
            send_sem=sent,
            recv_sem=arrived,
            device_id={"gx": ahead(1)},
            device_id_type=MESH,
        )

    def window(offset, corner, length, size):
        cell = lax.broadcasted_iota(jnp.int32, (length, size), 0).astype(F32) - corner
        total = jnp.zeros((length, size), F32)
        for d in range(6):
            total = jnp.where(cell == float(d), offset(d), total)
        return total

    for group, (begin, count) in enumerate(order.groups):
        all_of(send, recv, count - 1 + group, s1, r1.at[group]).wait_recv()
        base, amount = CAP * begin, CAP * count

        for g in range(GROUPS):
            block = recv[begin : begin + count, g, :]
            for i in range(PER_ROW):
                at = base + (i * GROUPS + g) * count
                lists[at : at + count, :] = block if i == 0 else pltpu.roll(block, 128 - 32 * i, 1)
        for start, size in chunks(amount, 128):
            lanes = slice(base + start, base + start + size)
            fields[:, lanes] = lists[lanes, :].T[0:32, :]
        for start, size in chunks(amount, 128):
            lanes = slice(base + start, base + start + size)
            zhi[:, lanes], zlo[:, lanes] = halves(
                window(lambda d: fields[24 + d : 25 + d, lanes], fields[5:6, lanes], cells_z, size)
            )
            wy[:, lanes] = window(
                lambda d: fields[16 + d : 17 + d, lanes], fields[4:5, lanes], cells_y, size
            )
            along = window(lambda d: fields[8 + d : 9 + d, lanes], fields[3:4, lanes], 16, size)
            for x in range(cells_x):
                wx[x, :, lanes] = jnp.broadcast_to(along[x : x + 1, :], (8, size))
            for c in range(3):
                tgt[c, :, lanes] = jnp.broadcast_to(fields[c : c + 1, lanes], (8, size))

        def sample(c, carry):
            at = pl.ds(c * cells_x * cells_y, cells_x * cells_y)
            for start, size in chunks(amount, 256):
                lanes = slice(base + start, base + start + size)
                along = nn(vhi[at, :], zhi[:, lanes])
                along = along + nn(vhi[at, :], zlo[:, lanes])
                along = along + nn(vlo[at, :], zhi[:, lanes])
                along = along.reshape(cells_x, cells_y // 8, 8, size)
                across = jnp.sum(along * wy[:, lanes].reshape(1, cells_y // 8, 8, size), axis=1)
                across = jnp.sum(across * wx[:, :, lanes], axis=0)
                force[c, :, lanes] = tgt[c, :, lanes] - jnp.sum(across, axis=0, keepdims=True)
            return carry

        lax.fori_loop(0, 3, sample, 0)

        for start, size in chunks(amount, 128):
            rows = slice(base + start, base + start + size)
            three = [force[c, 0:1, rows] for c in range(3)]
            three.append(jnp.zeros((125, size), F32))
            turned[rows, :] = jnp.concatenate(three, axis=0).T
        gathered = turned[base : base + count, :]
        for b in range(1, CAP):
            at = base + b * count
            gathered = gathered + pltpu.roll(turned[at : at + count, :], 8 * b, 1)
        back[begin : begin + count, 0, :] = gathered

    def answer(group, peer, mine, theirs):
        pltpu.make_async_remote_copy(
            src_ref=back.at[mine],
            dst_ref=returned.at[me],
            send_sem=s2,
            recv_sem=r2,
            device_id={"gx": peer},
            device_id_type=MESH,
        ).start()

    order.visit(me, answer)
    returned[pl.ds(me, 1)] = back[order.own : order.own + 1]

    def face_copy(source, halo, semaphore, to):
        return pltpu.make_async_remote_copy(
            src_ref=source,
            dst_ref=halo,
            send_sem=hs.at[semaphore],
            recv_sem=hr.at[semaphore],
            device_id=to,
            device_id_type=MESH,
        )

    sides = ((0, 0, 0), (1, cells_x - 1, cells_y - 1))
    near_copies, below_copies, above_copies = [], [], []
    for c in range(3):
        for side, x, y in sides:
            rows = slice(side * cells_y, (side + 1) * cells_y)
            box = wy[...].reshape(cells_y // 8, 8, slots) * (wx[x] * force[c])[None]
            ehi[c, rows, :], elo[c, rows, :] = halves(box.reshape(cells_y, slots))
        for x in range(cells_x):
            wxf[c, x : x + 1, :] = wx[x, 0:1, :] * force[c, 0:1, :]
        wxf[c, cells_x:, :] = jnp.zeros((YPAD - cells_x, slots), F32)
        for side, x, y in sides:
            rows = slice(2 * cells_y + YPAD * side, 2 * cells_y + YPAD * (side + 1))
            ehi[c, rows, :], elo[c, rows, :] = halves(wxf[c] * wy[y : y + 1, :])
        faces = nt(ehi[c], zhi[...]) + nt(ehi[c], zlo[...]) + nt(elo[c], zhi[...])
        for side, x, y in sides:
            rhs[c, x] = faces[side * cells_y : (side + 1) * cells_y] + v[c, x]
            at = 2 * cells_y + YPAD * side
            yedge[side, c, 0:cells_x, :] = faces[at : at + cells_x] + v[c, :, y, :]
            yedge[side, c, cells_x:, :] = jnp.zeros((YPAD - cells_x, cells_z), F32)
        down = face_copy(rhs.at[c, 0], xhalo.at[1, c], 4 * c, {"gx": ahead(n - 1)})
        up = face_copy(rhs.at[c, cells_x - 1], xhalo.at[0, c], 4 * c + 1, {"gx": ahead(1)})
        below = face_copy(
            yedge.at[0, c], yhalo.at[1, c], 4 * c + 2, {"gy": jnp.maximum(row - 1, 0)}
        )
        above = face_copy(
            yedge.at[1, c], yhalo.at[0, c], 4 * c + 3, {"gy": jnp.minimum(row + 1, ng - 1)}
        )
        down.start()
        up.start()
        near_copies += [down, up]
        below_copies.append(below)
        above_copies.append(above)

        @pl.when(row > 0)
        def _():
            below.start()

        @pl.when(row < ng - 1)
        def _():
            above.start()

    outward = [
        pltpu.make_async_copy(rhs.at[:, x], rhs_out.at[:, x], osem.at[i])
        for i, x in enumerate((0, cells_x - 1))
    ]
    for copy in outward:
        copy.start()

    def build(c, high, low):
        for x in range(inner):
            scaled = (wx[x + 1] * force[c])[None]
            box = (wy[...].reshape(cells_y // 8, 8, slots) * scaled).reshape(cells_y, slots)
            at = slice(x * cells_y, (x + 1) * cells_y)
            high[at, :], low[at, :] = halves(box)

    buffers = ((bhi0, blo0), (bhi1, blo1))
    build(0, *buffers[0])
    for c in range(3):
        high, low = buffers[c % 2]
        total = nt(high[...], zhi[...]) + nt(high[...], zlo[...]) + nt(low[...], zhi[...])
        rhs[c, 1 : cells_x - 1] = v[c, 1 : cells_x - 1] + total.reshape(inner, cells_y, cells_z)
        middle = pl.ds(1, inner)
        copy = pltpu.make_async_copy(rhs.at[c, middle], rhs_out.at[c, middle], osem.at[2 + c])
        copy.start()
        outward.append(copy)
        if c < 2:
            build(c + 1, *buffers[(c + 1) % 2])

    all_of(back, returned, n - 1, s2, r2).wait_recv()

    found = jnp.zeros((24, owned), F32)
    answers = returned[:, 0, :].T
    for i in range(PER_ROW):
        for g in range(GROUPS):
            b = i * GROUPS + g
            part = answers[8 * b : 8 * b + 8, :]
            first = part.astype(BF16).astype(F32)
            rest = part - first
            second = rest.astype(BF16).astype(F32)
            stack = jnp.concatenate([first, second, rest - second], axis=0).astype(BF16)
            found = found + nn(stack, onehot[b * n : (b + 1) * n, :])
    own[...] = found[0:8] + found[8:16] + found[16:24]
    copy = pltpu.make_async_copy(own, force_out, osem.at[5])
    copy.start()
    outward.append(copy)

    for copy in outward:
        copy.wait()
    all_of(send, recv, n - 1, s1, r1.at[0]).wait_send()
    all_of(back, returned, n - 1, s2, r2).wait_send()
    for copy in near_copies:
        copy.wait()

    @pl.when(row > 0)
    def _():
        for below, above in zip(below_copies, above_copies):
            below.wait_send()
            above.wait_recv()

    @pl.when(row < ng - 1)
    def _():
        for below, above in zip(below_copies, above_copies):
            above.wait_send()
            below.wait_recv()


def sweep_kernel(
    ng, rhs_in, xhalo_in, yhalo_in, force_in, out, force_out, rhs, xhalo, yhalo, force, made, lsem, sem
):
    row = lax.axis_index("gy")
    _, cells_x, cells_y, cells_z = rhs.shape
    part = cells_x // 2

    def halves_of(source, held, semaphores):
        return [
            pltpu.make_async_copy(
                source.at[c, pl.ds(h * part, part)], held.at[c, pl.ds(h * part, part)], semaphores.at[2 * c + h]
            )
            for c in range(3)
            for h in range(2)
        ]

    loads = halves_of(rhs_in, rhs, lsem)
    copies = halves_of(made, out, sem)
    rows_in = pltpu.make_async_copy(yhalo_in, yhalo, lsem.at[6])
    planes_in = pltpu.make_async_copy(xhalo_in, xhalo, lsem.at[7])
    last_in = pltpu.make_async_copy(force_in, force, lsem.at[8])
    for copy in (loads[0], rows_in, planes_in, *loads[1:], last_in):
        copy.start()
    line = lax.broadcasted_iota(jnp.int32, (cells_y, cells_z), 0)
    for c in range(3):
        loads[2 * c].wait()
        if c == 0:
            rows_in.wait()
        for turn, x in enumerate([*range(1, part - 1), 0, *range(part - 1, cells_x)]):
            if x == 0 and c == 0:
                planes_in.wait()
            if x == part - 1:
                loads[2 * c + 1].wait()
            here = rhs[c, x]
            total = xhalo[0, c] if x == 0 else rhs[c, x - 1]
            total = total + (xhalo[1, c] if x == cells_x - 1 else rhs[c, x + 1])
            total = total + pltpu.roll(here, 1, 1) + pltpu.roll(here, cells_z - 1, 1)
            lower = jnp.where(row == 0, 0.0, yhalo[0, c, x : x + 1, :])
            upper = jnp.where(row == ng - 1, 0.0, yhalo[1, c, x : x + 1, :])
            total = total + jnp.where(line == 0, lower, pltpu.roll(here, 1, 0))
            total = total + jnp.where(line == cells_y - 1, upper, pltpu.roll(here, cells_y - 1, 0))
            made[c, x] = (here + DIFFUSION * total) * (1.0 / (1.0 + 6.0 * DIFFUSION))
            if turn % part == part - 1:
                copies[2 * c + turn // part].start()
    last_in.wait()
    force_out[...] = force[0:3, :]
    for copy in copies:
        copy.wait()


def per_device(velocity, target, weights, corners, dest):
    n, ng = lax.axis_size("gx"), lax.axis_size("gy")
    _, cells_x, cells_y, cells_z = velocity.shape
    owned = target.shape[1]
    slots = CAP * n
    inner = cells_x - 2
    whole = pl.BlockSpec(memory_space=pltpu.VMEM)
    outside = pl.BlockSpec(memory_space=pltpu.HBM)
    vmem, dma = pltpu.VMEM, pltpu.SemaphoreType.DMA
    field = jax.ShapeDtypeStruct(velocity.shape, F32)
    flat = 3 * cells_x * cells_y
    edges = 2 * (cells_y + YPAD)
    rhs, xhalo, yhalo, force = pl.pallas_call(
        functools.partial(exchange_kernel, n, ng),
        out_shape=(
            field,
            jax.ShapeDtypeStruct((2, 3, cells_y, cells_z), F32),
            jax.ShapeDtypeStruct((2, 3, YPAD, cells_z), F32),
            jax.ShapeDtypeStruct((8, owned), F32),
        ),
        in_specs=[outside] * 5,
        out_specs=(outside,) * 4,
        scratch_shapes=[
            vmem(velocity.shape, F32),
            vmem(velocity.shape, F32),
            vmem((8, owned), F32),
            vmem(target.shape, F32),
            vmem(weights.shape, F32),
            vmem(corners.shape, jnp.int32),
            vmem((1, owned), jnp.int32),
            vmem((flat, cells_z), BF16),
            vmem((flat, cells_z), BF16),
            vmem((n, GROUPS, 128), F32),
            vmem((n, GROUPS, 128), F32),
            vmem((32, owned), F32),
            vmem((slots, owned), BF16),
            vmem((slots, 128), F32),
            vmem((32, slots), F32),
            vmem((cells_z, slots), BF16),
            vmem((cells_z, slots), BF16),
            vmem((cells_y, slots), F32),
            vmem((cells_x, 8, slots), F32),
            vmem((3, 8, slots), F32),
            vmem((3, 8, slots), F32),
            vmem((slots, 128), F32),
            vmem((n, 1, 128), F32),
            vmem((n, 1, 128), F32),
            vmem((3, edges, slots), BF16),
            vmem((3, edges, slots), BF16),
            vmem((3, YPAD, slots), F32),
            vmem((2, 3, YPAD, cells_z), F32),
            vmem((inner * cells_y, slots), BF16),
            vmem((inner * cells_y, slots), BF16),
            vmem((inner * cells_y, slots), BF16),
            vmem((inner * cells_y, slots), BF16),
            dma,
            dma((4,)),
            dma((6,)),
            dma,
            dma((2,)),
            dma,
            dma,
            dma((12,)),
            dma((12,)),
        ],
        compiler_params=pltpu.CompilerParams(
            collective_id=0, has_side_effects=True, vmem_limit_bytes=58000000
        ),
        name="exchange",
    )(velocity, target, weights, corners, dest.reshape(1, owned))
    return pl.pallas_call(
        functools.partial(sweep_kernel, ng),
        out_shape=(field, jax.ShapeDtypeStruct((3, owned), F32)),
        in_specs=[outside] * 4,
        out_specs=(outside, whole),
        scratch_shapes=[
            vmem(velocity.shape, F32),
            vmem((2, 3, cells_y, cells_z), F32),
            vmem((2, 3, YPAD, cells_z), F32),
            vmem((8, owned), F32),
            vmem(velocity.shape, F32),
            dma((9,)),
            dma((6,)),
        ],
        compiler_params=pltpu.CompilerParams(vmem_limit_bytes=58000000),
        name="sweep",
    )(rhs, xhalo, yhalo, force)


def solution(mesh):
    in_specs = (
        P(None, "gx", "gy", None),
        P(None, ("gx", "gy")),
        P(None, None, ("gx", "gy")),
        P(None, ("gx", "gy")),
        P(("gx", "gy"), None),
    )
    out_specs = (P(None, "gx", "gy", None), P(None, ("gx", "gy")))
    return jax.shard_map(
        per_device, mesh=mesh, in_specs=in_specs, out_specs=out_specs, check_vma=False
    )
```
